32 devices in a mesh: trial: 4 (over x, core), north: 2 (over y), east: 4 (over z).
Axes of the slice: x: 2, y: 2, z: 4, core: 2. Of those that a mesh axis runs over, the one named last changes fastest.
Arguments:
- pair_state: bfloat16 [192, 48, 128], P(('trial', 'north'), 'east'), parts along dimension 0, may hold values from -6 to 6
- in_gain: float32 [128], replicated, may hold values from 0.25 to 1.75
- left_weight: bfloat16 [512, 128], P('trial'), parts along dimension 0, may hold values from -0.5 to 0.5
- right_weight: bfloat16 [512, 128], P('trial'), parts along dimension 0, may hold values from -0.5 to 0.5
- left_gate: bfloat16 [512, 128], P('trial'), parts along dimension 0, may hold values from -0.5 to 0.5
- right_gate: bfloat16 [512, 128], P('trial'), parts along dimension 0, may hold values from -0.5 to 0.5
- mid_gain: float32 [128], replicated, may hold values from 0.25 to 1.75
- out_weight: bfloat16 [512, 128], P('trial'), parts along dimension 0, may hold values from -0.5 to 0.5
- out_gate: bfloat16 [512, 128], P('trial'), parts along dimension 0, may hold values from -0.5 to 0.5
Outputs:
- triangle_out: bfloat16 [192, 48, 128], P(('trial', 'north'), 'east'), parts along dimension 0
The draws below stay inside these ranges and needn't reach their ends.
There are 4 independent parts, one for each index of `trial`. The reference program is written for one: setup_inputs(seed, part) draws one part's arguments, and reference() takes and returns one part's arrays. A program takes and returns all parts, laid end to end along the dimension named above; an argument that names none is the same for every part. Nothing has to cross between parts.
All inputs are finite; a program needn't handle non-finite values.
Results may differ from the reference program's by a relative error of at most 0.015.
Values may be sent and summed in bfloat16 or wider, within the bound.
No kernel may reach another device: no remote copies, remote signals or barrier semaphores. Data moves between devices by JAX's collectives and lax.ppermute only.
A program may use at most 64 MiB of HBM per device.

```python
import jax
import jax.numpy as jnp
from jax import lax

RESIDUES = 48
PAIR_WIDTH = 128
MIX_WIDTH = 128


def block_scale(own_key, shape, pieces, low, top_value):
    def one(axis_at, blocks):
        draws = jax.random.uniform(jax.random.fold_in(jax.random.fold_in(own_key, 6), axis_at), (blocks,), jnp.float32, low / len(pieces), top_value / len(pieces))
        return jnp.repeat(jnp.exp(draws), shape[axis_at] // blocks).reshape((-1,) + (1,) * (len(shape) - axis_at - 1))

    level = one(*pieces[0])
    for cut in pieces[1:]:
        level = level * one(*cut)
    return level


def scatter_about(stream_key, shape, spread, reach, shards=(), kind=jnp.bfloat16):
    values = spread * jax.random.normal(stream_key, shape, jnp.float32)
    if shards:
        values = values * block_scale(stream_key, shape, shards, -0.22, 0.18)
    return jnp.clip(values, -reach, reach).astype(kind)


def setup_inputs(seed: int = 0, part: int = 0) -> dict:
    keys = jax.random.split(jax.random.key(seed), 10)
    own_keys = jax.random.split(jax.random.fold_in(keys[9], part), 10)
    pair_state = scatter_about(own_keys[0], (RESIDUES, RESIDUES, PAIR_WIDTH), 1.0, 6.0, ((0, 2), (1, 4)))
    in_gain = jnp.clip(1.0 + 0.15 * jax.random.normal(keys[1], (PAIR_WIDTH,), jnp.float32), 0.25, 1.75)
    left_weight = scatter_about(own_keys[2], (PAIR_WIDTH, MIX_WIDTH), PAIR_WIDTH ** -0.5, 0.5)
    right_weight = scatter_about(own_keys[3], (PAIR_WIDTH, MIX_WIDTH), PAIR_WIDTH ** -0.5, 0.5)
    left_gate = scatter_about(own_keys[4], (PAIR_WIDTH, MIX_WIDTH), PAIR_WIDTH ** -0.5, 0.5)
    right_gate = scatter_about(own_keys[5], (PAIR_WIDTH, MIX_WIDTH), PAIR_WIDTH ** -0.5, 0.5)
    mid_gain = jnp.clip(1.0 + 0.15 * jax.random.normal(keys[6], (MIX_WIDTH,), jnp.float32), 0.25, 1.75)
    out_weight = scatter_about(own_keys[7], (MIX_WIDTH, PAIR_WIDTH), MIX_WIDTH ** -0.5, 0.5)
    out_gate = scatter_about(own_keys[8], (PAIR_WIDTH, PAIR_WIDTH), PAIR_WIDTH ** -0.5, 0.5)
    return {"pair_state": pair_state, "in_gain": in_gain, "left_weight": left_weight, "right_weight": right_weight, "left_gate": left_gate, "right_gate": right_gate, "mid_gain": mid_gain, "out_weight": out_weight, "out_gate": out_gate}


def norm_channels(values, channel_gain):
    centred = values - lax.optimization_barrier(jnp.mean(values, axis=-1, keepdims=True))
    return centred * lax.rsqrt(lax.optimization_barrier(jnp.mean(centred * centred, axis=-1, keepdims=True)) + 1e-05) * channel_gain

def make_factors(pair_in, in_gain, left_weight, right_weight, left_gate, right_gate):
    ready = norm_channels(pair_in.astype(jnp.float32), in_gain).astype(jnp.bfloat16)
    ready = lax.optimization_barrier(ready)
    left = jnp.einsum('ijc,cd->ijd', ready.astype(jnp.float32), left_weight.astype(jnp.float32))
    left = left * jax.nn.sigmoid(jnp.einsum('ijc,cd->ijd', ready.astype(jnp.float32), left_gate.astype(jnp.float32)))
    right = jnp.einsum('ijc,cd->ijd', ready.astype(jnp.float32), right_weight.astype(jnp.float32))
    right = right * jax.nn.sigmoid(jnp.einsum('ijc,cd->ijd', ready.astype(jnp.float32), right_gate.astype(jnp.float32)))
    return (ready, left.astype(jnp.bfloat16), right.astype(jnp.bfloat16))

def to_pair(mixed, ready, mid_gain, out_weight, out_gate):
    scaled = norm_channels(mixed.astype(jnp.float32), mid_gain).astype(jnp.bfloat16)
    scaled = lax.optimization_barrier(scaled)
    gate = jax.nn.sigmoid(jnp.einsum('ijc,cd->ijd', ready.astype(jnp.float32), out_gate.astype(jnp.float32)))
    return (jnp.einsum('ijd,dc->ijc', scaled.astype(jnp.float32), out_weight.astype(jnp.float32)) * gate).astype(jnp.bfloat16)

def reference(pair_state, in_gain, left_weight, right_weight, left_gate, right_gate, mid_gain, out_weight, out_gate):
    ready, left, right = make_factors(pair_state, in_gain, left_weight, right_weight, left_gate, right_gate)
    left, right = lax.optimization_barrier((left, right))

    def one_channel(pair_of):
        return (jnp.dot(pair_of[0], pair_of[1].T, preferred_element_type=jnp.float32) * RESIDUES ** (-0.5)).astype(jnp.bfloat16)
    mixed = jnp.moveaxis(lax.map(one_channel, (jnp.moveaxis(left, -1, 0), jnp.moveaxis(right, -1, 0))), 0, -1)
    mixed = lax.optimization_barrier(mixed)
    return to_pair(mixed, ready, mid_gain, out_weight, out_gate)
```

```python
import functools

import jax
import jax.numpy as jnp
from jax import lax
from jax.experimental import pallas as pl
from jax.experimental.pallas import tpu as pltpu
from jax.sharding import PartitionSpec as P

def norm_channels(values, channel_gain):
    centred = values - jnp.mean(values, axis=-1, keepdims=True)
    return (
        centred
        * lax.rsqrt(jnp.mean(centred * centred, axis=-1, keepdims=True) + 1e-05)
        * channel_gain
    )


def make_factors(pair_in, in_gain, left_weight, right_weight, left_gate, right_gate):
    ready = norm_channels(pair_in.astype(jnp.float32), in_gain).astype(jnp.bfloat16)
    ready = lax.optimization_barrier(ready)
    left = jnp.einsum("ijc,cd->ijd", ready, left_weight, preferred_element_type=jnp.float32)
    left = left * jax.nn.sigmoid(
        jnp.einsum("ijc,cd->ijd", ready, left_gate, preferred_element_type=jnp.float32)
    )
    right = jnp.einsum("ijc,cd->ijd", ready, right_weight, preferred_element_type=jnp.float32)
    right = right * jax.nn.sigmoid(
        jnp.einsum("ijc,cd->ijd", ready, right_gate, preferred_element_type=jnp.float32)
    )
    return (ready, left.astype(jnp.bfloat16), right.astype(jnp.bfloat16))


def to_pair(mixed, ready, mid_gain, out_weight, out_gate):
    scaled = norm_channels(mixed.astype(jnp.float32), mid_gain).astype(jnp.bfloat16)
    scaled = lax.optimization_barrier(scaled)
    gate = jax.nn.sigmoid(
        jnp.einsum("ijc,cd->ijd", ready, out_gate, preferred_element_type=jnp.float32)
    )
    return (
        jnp.einsum("ijd,dc->ijc", scaled, out_weight, preferred_element_type=jnp.float32) * gate
    ).astype(jnp.bfloat16)


def local_lines(
    pair_state,
    in_gain,
    left_weight,
    right_weight,
    left_gate,
    right_gate,
    mid_gain,
    out_weight,
    out_gate,
):
    ready, left, right = make_factors(
        pair_state, in_gain, left_weight, right_weight, left_gate, right_gate
    )
    count = pair_state.shape[1] * lax.axis_size("east")
    left_lines, right_lines = (
        lax.all_to_all(left, "east", split_axis=2, concat_axis=1, tiled=True),
        lax.all_to_all(right, "east", split_axis=2, concat_axis=1, tiled=True),
    )
    strip = jnp.einsum(
        "ikd,jkd->ijd",
        left_lines,
        lax.all_gather(right_lines, "north", axis=0, tiled=True),
        preferred_element_type=jnp.float32,
    )
    strip = (strip * count ** (-0.5)).astype(jnp.bfloat16)
    mixed = lax.all_to_all(strip, "east", split_axis=1, concat_axis=2, tiled=True)
    return to_pair(mixed, ready, mid_gain, out_weight, out_gate)


ROW_TILE = 8


def dot32(a, b):
    return jnp.dot(a, b, preferred_element_type=jnp.float32)


def windows(rows, cols):
    halves = rows // cols
    starts = [h * cols // ROW_TILE * ROW_TILE for h in range(halves)]
    width = max(-(-(h * cols + cols - starts[h]) // ROW_TILE) * ROW_TILE for h in range(halves))
    if rows % ROW_TILE or any(start + width > rows for start in starts):
        starts = [h * cols for h in range(halves)]
        width = cols
    return starts, width


def gated(ready, weight, gate):
    both = dot32(ready, jnp.concatenate([weight[...], gate[...]], axis=1))
    width = both.shape[1] // 2
    value = both[:, :width] * jax.nn.sigmoid(both[:, width:])
    return value.astype(jnp.bfloat16).astype(jnp.float32)


def triangle_kernel(
    place, *refs, blocks, starts, width, rows, cols, scale
):
    own = refs[:blocks]
    far = refs[blocks : 2 * blocks]
    (
        in_gain,
        left_weight,
        right_weight,
        left_gate,
        right_gate,
        mid_gain,
        out_weight,
        out_gate,
        out,
        left,
        right,
    ) = refs[2 * blocks :]
    same = place[0] == 1
    half = place[1]
    channels = out.shape[-1]
    gain = in_gain[...]
    keep = None
    for b in range(blocks):
        flat = own[b][...].astype(jnp.float32).reshape(cols * rows, channels)
        ready = norm_channels(flat, gain).astype(jnp.bfloat16)
        if b == 0:
            keep = ready
        left[pl.ds(b * cols, cols)] = gated(ready, left_weight, left_gate).reshape(
            cols, rows, channels
        )
        window = own[b][:, starts[0] : starts[0] + width].astype(jnp.float32)
        for h in range(1, len(starts)):
            window = jnp.where(
                half == h,
                own[b][:, starts[h] : starts[h] + width].astype(jnp.float32),
                window,
            )
        window = jnp.where(same, window, far[-b % blocks][...].astype(jnp.float32))
        ready = norm_channels(window.reshape(cols * width, channels), gain).astype(jnp.bfloat16)
        right[pl.ds(b * cols, cols)] = gated(ready, right_weight, right_gate).reshape(
            cols, width, channels
        )
    offset = place[2]

    def step(k, sums):
        line = left[k]
        return tuple(
            sums[j] + line * right[k, pl.ds(offset + j, 1), :] for j in range(cols)
        )

    sums = lax.fori_loop(
        0,
        blocks * cols,
        step,
        tuple(jnp.zeros((rows, channels), jnp.float32) for _ in range(cols)),
        unroll=4,
    )
    mixed = jnp.concatenate([(part * scale).astype(jnp.bfloat16) for part in sums], axis=0)
    scaled = norm_channels(mixed.astype(jnp.float32), mid_gain[...]).astype(jnp.bfloat16)
    result = dot32(scaled, out_weight[...]) * jax.nn.sigmoid(dot32(keep, out_gate[...]))
    out[...] = result.astype(jnp.bfloat16).reshape(cols, rows, channels)


def local_gather(
    pair_state,
    in_gain,
    left_weight,
    right_weight,
    left_gate,
    right_gate,
    mid_gain,
    out_weight,
    out_gate,
    *,
    north,
    east,
):
    block = jnp.transpose(pair_state, (1, 0, 2))
    cols, rows, channels = block.shape
    halves = rows // cols
    starts, width = windows(rows, cols)
    n = lax.axis_index("north")
    e = lax.axis_index("east")
    order = sorted(range(1, east), key=lambda s: -min(s, east - s))
    own = [block] + [None] * (east - 1)
    for s in order:
        own[s] = lax.ppermute(block, "east", [(i, (i + s) % east) for i in range(east)])
    far = []
    for r in range(east):
        send = block[:, starts[0] : starts[0] + width]
        for h in range(1, halves):
            send = jnp.where(
                (e - halves * n - r) % east == h,
                block[:, starts[h] : starts[h] + width],
                send,
            )
        pairs = [
            (m * east + (halves * m + h + r) % east, (1 - m) * east + halves * m + h)
            for m in range(north)
            for h in range(halves)
        ]
        far.append(lax.ppermute(send, ("north", "east"), pairs))
    half = e % halves
    same = (e // halves == n).astype(jnp.int32)
    offset = half * cols - jnp.asarray(starts, jnp.int32)[half]
    place = jnp.stack([same, half, offset]).astype(jnp.int32)
    kernel = functools.partial(
        triangle_kernel,
        blocks=east,
        starts=starts,
        width=width,
        rows=rows,
        cols=cols,
        scale=(cols * east) ** (-0.5),
    )
    result = pl.pallas_call(
        kernel,
        out_shape=jax.ShapeDtypeStruct((cols, rows, channels), jnp.bfloat16),
        in_specs=[pl.BlockSpec(memory_space=pltpu.SMEM)]
        + [pl.BlockSpec(memory_space=pltpu.VMEM)] * (2 * east + 8),
        out_specs=pl.BlockSpec(memory_space=pltpu.VMEM),
        scratch_shapes=[
            pltpu.VMEM((cols * east, rows, channels), jnp.float32),
            pltpu.VMEM((cols * east, width, channels), jnp.float32),
        ],
    )(
        place,
        *own,
        *far,
        in_gain[None],
        left_weight,
        right_weight,
        left_gate,
        right_gate,
        mid_gain[None],
        out_weight,
        out_gate,
    )
    return jnp.transpose(result, (1, 0, 2))


def pick_local(pair_state, *rest, north, east):
    rows, cols, _ = pair_state.shape
    small = pair_state.size * pair_state.dtype.itemsize * east <= 2**21
    if small and north == 2 and rows % cols == 0 and east * cols == north * rows:
        return local_gather(pair_state, *rest, north=north, east=east)
    return local_lines(pair_state, *rest)


def solution(mesh):
    return jax.shard_map(
        functools.partial(pick_local, north=mesh.shape["north"], east=mesh.shape["east"]),
        mesh=mesh,
        in_specs=(
            P(("trial", "north"), "east", None),
            P(),
            P("trial", None),
            P("trial", None),
            P("trial", None),
            P("trial", None),
            P(),
            P("trial", None),
            P("trial", None),
        ),
        out_specs=P(("trial", "north"), "east", None),
        check_vma=False,
    )
```

```python
import functools

import jax
import jax.numpy as jnp
from jax import lax
from jax.experimental import pallas as pl
from jax.experimental.pallas import tpu as pltpu
from jax.sharding import PartitionSpec as P


def norm_channels(values, channel_gain):
    centred = values - jnp.mean(values, axis=-1, keepdims=True)
    return (
        centred
        * lax.rsqrt(jnp.mean(centred * centred, axis=-1, keepdims=True) + 1e-05)
        * channel_gain
    )


def make_factors(pair_in, in_gain, left_weight, right_weight, left_gate, right_gate):
    ready = norm_channels(pair_in.astype(jnp.float32), in_gain).astype(jnp.bfloat16)
    ready = lax.optimization_barrier(ready)
    left = jnp.einsum("ijc,cd->ijd", ready, left_weight, preferred_element_type=jnp.float32)
    left = left * jax.nn.sigmoid(
        jnp.einsum("ijc,cd->ijd", ready, left_gate, preferred_element_type=jnp.float32)
    )
    right = jnp.einsum("ijc,cd->ijd", ready, right_weight, preferred_element_type=jnp.float32)
    right = right * jax.nn.sigmoid(
        jnp.einsum("ijc,cd->ijd", ready, right_gate, preferred_element_type=jnp.float32)
    )
    return (ready, left.astype(jnp.bfloat16), right.astype(jnp.bfloat16))


def to_pair(mixed, ready, mid_gain, out_weight, out_gate):
    scaled = norm_channels(mixed.astype(jnp.float32), mid_gain).astype(jnp.bfloat16)
    scaled = lax.optimization_barrier(scaled)
    gate = jax.nn.sigmoid(
        jnp.einsum("ijc,cd->ijd", ready, out_gate, preferred_element_type=jnp.float32)
    )
    return (
        jnp.einsum("ijd,dc->ijc", scaled, out_weight, preferred_element_type=jnp.float32) * gate
    ).astype(jnp.bfloat16)


def local_lines(
    pair_state,
    in_gain,
    left_weight,
    right_weight,
    left_gate,
    right_gate,
    mid_gain,
    out_weight,
    out_gate,
):
    ready, left, right = make_factors(
        pair_state, in_gain, left_weight, right_weight, left_gate, right_gate
    )
    count = pair_state.shape[1] * lax.axis_size("east")
    left_lines, right_lines = (
        lax.all_to_all(left, "east", split_axis=2, concat_axis=1, tiled=True),
        lax.all_to_all(right, "east", split_axis=2, concat_axis=1, tiled=True),
    )
    strip = jnp.einsum(
        "ikd,jkd->ijd",
        left_lines,
        lax.all_gather(right_lines, "north", axis=0, tiled=True),
        preferred_element_type=jnp.float32,
    )
    strip = (strip * count ** (-0.5)).astype(jnp.bfloat16)
    mixed = lax.all_to_all(strip, "east", split_axis=1, concat_axis=2, tiled=True)
    return to_pair(mixed, ready, mid_gain, out_weight, out_gate)


def dot32(a, b):
    return jnp.dot(a, b, preferred_element_type=jnp.float32)


def ready_of(block, gain):
    cols, rows, channels = block.shape
    flat = block.astype(jnp.float32).reshape(cols * rows, channels)
    return norm_channels(flat, gain[...]).astype(jnp.bfloat16)


def gated(ready, weight, gate, shape):
    both = dot32(ready, jnp.concatenate([weight[...], gate[...]], axis=1))
    width = both.shape[1] // 2
    value = both[:, :width] * jax.nn.sigmoid(both[:, width:])
    return value.astype(jnp.bfloat16).astype(jnp.float32).reshape(shape)


def same_rows(tiles):
    return lax.axis_index("east") // tiles == lax.axis_index("north")


def add_lines(left, right, first, begin, group):
    lines, _, _ = left.shape

    def step(k, sums):
        line = left[k]
        return tuple(
            sums[j] + line * right[k, begin + j : begin + j + 1, :] for j in range(group)
        )

    return lax.fori_loop(0, lines, step, first, unroll=4)


def near_kernel(
    own, own_other, far, in_gain, left_weight, right_weight, left_gate, right_gate, out_gate,
    sums, far_left, gate, left, right, *, tiles
):
    cols, rows, channels = own.shape
    ready = ready_of(own[...], in_gain)
    left[...] = gated(ready, left_weight, left_gate, own.shape)
    gate[...] = jax.nn.sigmoid(dot32(ready, out_gate[...])).reshape(own.shape)
    source = jnp.where(same_rows(tiles), own[...].astype(jnp.float32), own_other[...].astype(jnp.float32))
    right[...] = gated(ready_of(source, in_gain), right_weight, right_gate, own.shape)
    zero = jnp.zeros((rows, channels), jnp.float32)
    for begin in range(0, rows, cols):
        for j, part in enumerate(add_lines(left, right, (zero,) * cols, begin, cols)):
            sums[begin + j] = part
    far_left[...] = gated(ready_of(far[...], in_gain), left_weight, left_gate, own.shape)


def far_kernel(
    far, far_other, far_left, sums, in_gain, right_weight, right_gate, keep, send, right, total,
    *, tiles
):
    cols, rows, _ = far.shape
    source = jnp.where(same_rows(tiles), far[...].astype(jnp.float32), far_other[...].astype(jnp.float32))
    right[...] = gated(ready_of(source, in_gain), right_weight, right_gate, far.shape)
    for begin in range(0, rows, cols):
        first = tuple(sums[begin + j] for j in range(cols))
        for j, part in enumerate(add_lines(far_left, right, first, begin, cols)):
            total[begin + j] = part
    tile = lax.axis_index("east") % tiles
    keep[...] = total[pl.ds(tile * cols, cols)]
    send[...] = total[pl.ds((tiles - 1 - tile) * cols, cols)].astype(jnp.bfloat16)


def last_kernel(keep, other, gate, mid_gain, out_weight, out, *, scale):
    total = keep[...] + other[...].astype(jnp.float32)
    mixed = (total * scale).astype(jnp.bfloat16)
    scaled = ready_of(mixed, mid_gain)
    result = dot32(scaled, out_weight[...]).reshape(out.shape) * gate[...]
    out[...] = result.astype(jnp.bfloat16)


def kernel_call(kernel, args, outs, scratch=()):
    whole = pl.BlockSpec(memory_space=pltpu.VMEM)
    return pl.pallas_call(
        kernel,
        out_shape=outs,
        in_specs=[whole] * len(args),
        out_specs=jax.tree.map(lambda _: whole, outs),
        scratch_shapes=list(scratch),
    )(*args)


def local_halves(
    pair_state,
    in_gain,
    left_weight,
    right_weight,
    left_gate,
    right_gate,
    mid_gain,
    out_weight,
    out_gate,
    *,
    north,
    east,
):
    tiles = east // north
    own = jnp.transpose(pair_state, (1, 0, 2))
    cols, rows, channels = own.shape
    across = [(e, (e + tiles) % east) for e in range(east)]
    beside = [(e, e // tiles * tiles + tiles - 1 - e % tiles) for e in range(east)]
    over = [(n, north - 1 - n) for n in range(north)]
    wide = jax.ShapeDtypeStruct(own.shape, jnp.float32)
    square = jax.ShapeDtypeStruct((rows, rows, channels), jnp.float32)
    slim = jax.ShapeDtypeStruct(own.shape, jnp.bfloat16)
    in_gain = in_gain[None]
    far = lax.ppermute(own, "east", across)
    own_other = lax.ppermute(own, "north", over)
    far_other = lax.ppermute(far, "north", over)
    sums, far_left, gate = kernel_call(
        functools.partial(near_kernel, tiles=tiles),
        (own, own_other, far, in_gain, left_weight, right_weight, left_gate, right_gate, out_gate),
        (square, wide, wide),
        (pltpu.VMEM(own.shape, jnp.float32), pltpu.VMEM(own.shape, jnp.float32)),
    )
    keep, send = kernel_call(
        functools.partial(far_kernel, tiles=tiles),
        (far, far_other, far_left, sums, in_gain, right_weight, right_gate),
        (wide, slim),
        (pltpu.VMEM(own.shape, jnp.float32), pltpu.VMEM(square.shape, jnp.float32)),
    )
    other = lax.ppermute(send, "east", beside)
    result = kernel_call(
        functools.partial(last_kernel, scale=(cols * east) ** (-0.5)),
        (keep, other, gate, mid_gain[None], out_weight),
        slim,
    )
    return jnp.transpose(result, (1, 0, 2))


def pick_local(pair_state, *rest, north, east):
    rows, cols, _ = pair_state.shape
    small = pair_state.size * pair_state.dtype.itemsize * east <= 2**21
    if small and north == 2 and east == 2 * north and rows == 2 * cols:
        return local_halves(pair_state, *rest, north=north, east=east)
    return local_lines(pair_state, *rest)


def solution(mesh):
    return jax.shard_map(
        functools.partial(pick_local, north=mesh.shape["north"], east=mesh.shape["east"]),
        mesh=mesh,
        in_specs=(
            P(("trial", "north"), "east", None),
            P(),
            P("trial", None),
            P("trial", None),
            P("trial", None),
            P("trial", None),
            P(),
            P("trial", None),
            P("trial", None),
        ),
        out_specs=P(("trial", "north"), "east", None),
        check_vma=False,
    )
```

```python
import functools

import jax
import jax.numpy as jnp
from jax import lax
from jax.experimental import pallas as pl
from jax.experimental.pallas import tpu as pltpu
from jax.sharding import PartitionSpec as P


def norm_channels(values, channel_gain):
    centred = values - jnp.mean(values, axis=-1, keepdims=True)
    return (
        centred
        * lax.rsqrt(jnp.mean(centred * centred, axis=-1, keepdims=True) + 1e-05)
        * channel_gain
    )


def make_factors(pair_in, in_gain, left_weight, right_weight, left_gate, right_gate):
    ready = norm_channels(pair_in.astype(jnp.float32), in_gain).astype(jnp.bfloat16)
    ready = lax.optimization_barrier(ready)
    left = jnp.einsum("ijc,cd->ijd", ready, left_weight, preferred_element_type=jnp.float32)
    left = left * jax.nn.sigmoid(
        jnp.einsum("ijc,cd->ijd", ready, left_gate, preferred_element_type=jnp.float32)
    )
    right = jnp.einsum("ijc,cd->ijd", ready, right_weight, preferred_element_type=jnp.float32)
    right = right * jax.nn.sigmoid(
        jnp.einsum("ijc,cd->ijd", ready, right_gate, preferred_element_type=jnp.float32)
    )
    return (ready, left.astype(jnp.bfloat16), right.astype(jnp.bfloat16))


def to_pair(mixed, ready, mid_gain, out_weight, out_gate):
    scaled = norm_channels(mixed.astype(jnp.float32), mid_gain).astype(jnp.bfloat16)
    scaled = lax.optimization_barrier(scaled)
    gate = jax.nn.sigmoid(
        jnp.einsum("ijc,cd->ijd", ready, out_gate, preferred_element_type=jnp.float32)
    )
    return (
        jnp.einsum("ijd,dc->ijc", scaled, out_weight, preferred_element_type=jnp.float32) * gate
    ).astype(jnp.bfloat16)


def local_lines(
    pair_state,
    in_gain,
    left_weight,
    right_weight,
    left_gate,
    right_gate,
    mid_gain,
    out_weight,
    out_gate,
):
    ready, left, right = make_factors(
        pair_state, in_gain, left_weight, right_weight, left_gate, right_gate
    )
    count = pair_state.shape[1] * lax.axis_size("east")
    left_lines, right_lines = (
        lax.all_to_all(left, "east", split_axis=2, concat_axis=1, tiled=True),
        lax.all_to_all(right, "east", split_axis=2, concat_axis=1, tiled=True),
    )
    strip = jnp.einsum(
        "ikd,jkd->ijd",
        left_lines,
        lax.all_gather(right_lines, "north", axis=0, tiled=True),
        preferred_element_type=jnp.float32,
    )
    strip = (strip * count ** (-0.5)).astype(jnp.bfloat16)
    mixed = lax.all_to_all(strip, "east", split_axis=1, concat_axis=2, tiled=True)
    return to_pair(mixed, ready, mid_gain, out_weight, out_gate)


def dot32(a, b):
    return jnp.dot(a, b, preferred_element_type=jnp.float32)


def ready_of(block, gain):
    cols, rows, channels = block.shape
    flat = block.astype(jnp.float32).reshape(cols * rows, channels)
    return norm_channels(flat, gain[...]).astype(jnp.bfloat16)


def gated(ready, pair, shape):
    both = dot32(ready, pair[...])
    width = both.shape[1] // 2
    value = both[:, :width] * jax.nn.sigmoid(both[:, width:])
    return value.astype(jnp.bfloat16).astype(jnp.float32).reshape(shape)


def same_rows(tiles):
    return lax.axis_index("east") // tiles == lax.axis_index("north")


def add_lines(left, right, first, begin, group):
    lines, _, _ = left.shape

    def step(k, sums):
        line = left[k]
        return tuple(
            sums[j] + line * right[k, begin + j : begin + j + 1, :] for j in range(group)
        )

    return lax.fori_loop(0, lines, step, first, unroll=4)


def own_kernel(
    own, in_gain, left_weight, right_weight, left_gate, right_gate, mid_gain, out_weight, out_gate,
    left, right, gate, left_pair, right_pair, out_copy, in_copy, mid_copy
):
    channels = left_weight.shape[1]
    left_pair[:, :channels] = left_weight[...]
    left_pair[:, channels:] = left_gate[...]
    right_pair[:, :channels] = right_weight[...]
    right_pair[:, channels:] = right_gate[...]
    out_copy[...] = out_weight[...]
    in_copy[...] = in_gain[...]
    mid_copy[...] = mid_gain[...]
    ready = ready_of(own[...], in_gain)
    left[...] = gated(ready, left_pair, own.shape)
    right[...] = gated(ready, right_pair, own.shape)
    gate[...] = jax.nn.sigmoid(dot32(ready, out_gate[...])).reshape(own.shape)


def near_kernel(
    left, own_right, own_other, far, in_gain, left_pair, right_pair,
    sums, far_left, far_right, right, *, tiles
):
    cols, rows, channels = left.shape
    same = same_rows(tiles)

    @pl.when(same)
    def _():
        right[...] = own_right[...]
        far_right[...] = gated(ready_of(far[...], in_gain), right_pair, left.shape)

    @pl.when(jnp.logical_not(same))
    def _():
        right[...] = gated(ready_of(own_other[...], in_gain), right_pair, left.shape)

    zero = jnp.zeros((rows, channels), jnp.float32)
    for begin in range(0, rows, cols):
        for j, part in enumerate(add_lines(left, right, (zero,) * cols, begin, cols)):
            sums[begin + j] = part
    far_left[...] = gated(ready_of(far[...], in_gain), left_pair, left.shape)


def far_kernel(
    far_other, far_left, far_right, sums, in_gain, right_pair, keep, send, right, total, *, tiles
):
    cols, rows, _ = far_left.shape
    same = same_rows(tiles)

    @pl.when(same)
    def _():
        right[...] = far_right[...]

    @pl.when(jnp.logical_not(same))
    def _():
        right[...] = gated(ready_of(far_other[...], in_gain), right_pair, far_left.shape)

    for begin in range(0, rows, cols):
        first = tuple(sums[begin + j] for j in range(cols))
        for j, part in enumerate(add_lines(far_left, right, first, begin, cols)):
            total[begin + j] = part
    tile = lax.axis_index("east") % tiles
    keep[...] = total[pl.ds(tile * cols, cols)]
    send[...] = total[pl.ds((tiles - 1 - tile) * cols, cols)].astype(jnp.bfloat16)


def last_kernel(keep, other, gate, mid_gain, out_weight, out, *, scale):
    total = keep[...] + other[...].astype(jnp.float32)
    mixed = (total * scale).astype(jnp.bfloat16)
    scaled = ready_of(mixed, mid_gain)
    result = dot32(scaled, out_weight[...]).reshape(out.shape) * gate[...]
    out[...] = result.astype(jnp.bfloat16)


def kernel_call(kernel, args, outs, scratch=(), first=False, last=False):
    whole = pl.BlockSpec(memory_space=pltpu.VMEM)
    if not last:
        outs = jax.tree.map(lambda leaf: pltpu.VMEM(leaf.shape, leaf.dtype), outs)
    if not first:
        args = [pltpu.with_memory_space_constraint(arg, pltpu.VMEM) for arg in args]
    return pl.pallas_call(
        kernel,
        out_shape=outs,
        in_specs=[whole] * len(args),
        out_specs=jax.tree.map(lambda _: whole, outs),
        scratch_shapes=list(scratch),
    )(*args)


def local_halves(
    pair_state,
    in_gain,
    left_weight,
    right_weight,
    left_gate,
    right_gate,
    mid_gain,
    out_weight,
    out_gate,
    *,
    north,
    east,
):
    tiles = east // north
    own = jnp.transpose(pair_state, (1, 0, 2))
    cols, rows, channels = own.shape
    across = [(e, (e + tiles) % east) for e in range(east)]
    beside = [(e, e // tiles * tiles + tiles - 1 - e % tiles) for e in range(east)]
    over = [(n, north - 1 - n) for n in range(north)]
    wide = jax.ShapeDtypeStruct(own.shape, jnp.float32)
    square = jax.ShapeDtypeStruct((rows, rows, channels), jnp.float32)
    slim = jax.ShapeDtypeStruct(own.shape, jnp.bfloat16)
    line = jax.ShapeDtypeStruct((1, channels), jnp.float32)
    weight = jax.ShapeDtypeStruct(out_weight.shape, jnp.bfloat16)
    double = jax.ShapeDtypeStruct((channels, 2 * channels), jnp.bfloat16)
    far = lax.ppermute(own, "east", across)
    own_other = lax.ppermute(own, "north", over)
    far_other = lax.ppermute(far, "north", over)
    left, right, gate, left_pair, right_pair, out_copy, in_copy, mid_copy = kernel_call(
        own_kernel,
        (own, in_gain[None], left_weight, right_weight, left_gate, right_gate)
        + (mid_gain[None], out_weight, out_gate),
        (wide, wide, wide, double, double, weight, line, line),
        first=True,
    )
    sums, far_left, far_right = kernel_call(
        functools.partial(near_kernel, tiles=tiles),
        (left, right, own_other, far, in_copy, left_pair, right_pair),
        (square, wide, wide),
        (pltpu.VMEM(own.shape, jnp.float32),),
    )
    keep, send = kernel_call(
        functools.partial(far_kernel, tiles=tiles),
        (far_other, far_left, far_right, sums, in_copy, right_pair),
        (wide, slim),
        (pltpu.VMEM(own.shape, jnp.float32), pltpu.VMEM(square.shape, jnp.float32)),
    )
    other = lax.ppermute(send, "east", beside)
    result = kernel_call(
        functools.partial(last_kernel, scale=(cols * east) ** (-0.5)),
        (keep, other, gate, mid_copy, out_copy),
        slim,
        last=True,
    )
    return jnp.transpose(result, (1, 0, 2))


def takes_halves(north, east):
    return north == 2 and east == 2 * north


def pick_local(pair_state, *rest, north, east):
    rows, cols, _ = pair_state.shape
    small = pair_state.size * pair_state.dtype.itemsize * east <= 2**21
    if small and takes_halves(north, east) and rows == 2 * cols:
        return local_halves(pair_state, *rest, north=north, east=east)
    return local_lines(pair_state, *rest)


def solution(mesh):
    return jax.shard_map(
        functools.partial(pick_local, north=mesh.shape["north"], east=mesh.shape["east"]),
        mesh=mesh,
        in_specs=(
            P(("trial", "north"), "east", None),
            P(),
            P("trial", None),
            P("trial", None),
            P("trial", None),
            P("trial", None),
            P(),
            P("trial", None),
            P("trial", None),
        ),
        out_specs=P(("trial", "north"), "east", None),
        check_vma=False,
    )
```

```python
import functools

import jax
import jax.numpy as jnp
from jax import lax
from jax.experimental import pallas as pl
from jax.experimental.pallas import tpu as pltpu
from jax.sharding import PartitionSpec as P


def norm_channels(values, channel_gain):
    centred = values - jnp.mean(values, axis=-1, keepdims=True)
    return (
        centred
        * lax.rsqrt(jnp.mean(centred * centred, axis=-1, keepdims=True) + 1e-05)
        * channel_gain
    )


def make_factors(pair_in, in_gain, left_weight, right_weight, left_gate, right_gate):
    ready = norm_channels(pair_in.astype(jnp.float32), in_gain).astype(jnp.bfloat16)
    ready = lax.optimization_barrier(ready)
    left = jnp.einsum("ijc,cd->ijd", ready, left_weight, preferred_element_type=jnp.float32)
    left = left * jax.nn.sigmoid(
        jnp.einsum("ijc,cd->ijd", ready, left_gate, preferred_element_type=jnp.float32)
    )
    right = jnp.einsum("ijc,cd->ijd", ready, right_weight, preferred_element_type=jnp.float32)
    right = right * jax.nn.sigmoid(
        jnp.einsum("ijc,cd->ijd", ready, right_gate, preferred_element_type=jnp.float32)
    )
    return (ready, left.astype(jnp.bfloat16), right.astype(jnp.bfloat16))


def to_pair(mixed, ready, mid_gain, out_weight, out_gate):
    scaled = norm_channels(mixed.astype(jnp.float32), mid_gain).astype(jnp.bfloat16)
    scaled = lax.optimization_barrier(scaled)
    gate = jax.nn.sigmoid(
        jnp.einsum("ijc,cd->ijd", ready, out_gate, preferred_element_type=jnp.float32)
    )
    return (
        jnp.einsum("ijd,dc->ijc", scaled, out_weight, preferred_element_type=jnp.float32) * gate
    ).astype(jnp.bfloat16)


def local_lines(
    pair_state,
    in_gain,
    left_weight,
    right_weight,
    left_gate,
    right_gate,
    mid_gain,
    out_weight,
    out_gate,
):
    ready, left, right = make_factors(
        pair_state, in_gain, left_weight, right_weight, left_gate, right_gate
    )
    count = pair_state.shape[1] * lax.axis_size("east")
    left_lines, right_lines = (
        lax.all_to_all(left, "east", split_axis=2, concat_axis=1, tiled=True),
        lax.all_to_all(right, "east", split_axis=2, concat_axis=1, tiled=True),
    )
    strip = jnp.einsum(
        "ikd,jkd->ijd",
        left_lines,
        lax.all_gather(right_lines, "north", axis=0, tiled=True),
        preferred_element_type=jnp.float32,
    )
    strip = (strip * count ** (-0.5)).astype(jnp.bfloat16)
    mixed = lax.all_to_all(strip, "east", split_axis=1, concat_axis=2, tiled=True)
    return to_pair(mixed, ready, mid_gain, out_weight, out_gate)


def dot32(a, b):
    return jnp.dot(a, b, preferred_element_type=jnp.float32)


def ready_of(block, gain):
    cols, rows, channels = block.shape
    flat = block.astype(jnp.float32).reshape(cols * rows, channels)
    return norm_channels(flat, gain[...]).astype(jnp.bfloat16)


def gated(ready, pair, shape):
    both = dot32(ready, pair[...])
    width = both.shape[1] // 2
    value = both[:, :width] * jax.nn.sigmoid(both[:, width:])
    return value.astype(jnp.bfloat16).astype(jnp.float32).reshape(shape)


def same_rows(tiles):
    return lax.axis_index("east") // tiles == lax.axis_index("north")


def add_lines(left, right, first, begin, group):
    lines, _, _ = left.shape

    def step(k, sums):
        line = left[k]
        return tuple(
            sums[j] + line * right[k, begin + j : begin + j + 1, :] for j in range(group)
        )

    return lax.fori_loop(0, lines, step, first, unroll=4)


def own_kernel(
    own, in_gain, left_weight, right_weight, left_gate, right_gate, mid_gain, out_weight, out_gate,
    left, right, gate, left_pair, right_pair, out_copy, in_copy, mid_copy
):
    channels = left_weight.shape[1]
    left_pair[:, :channels] = left_weight[...]
    left_pair[:, channels:] = left_gate[...]
    right_pair[:, :channels] = right_weight[...]
    right_pair[:, channels:] = right_gate[...]
    out_copy[...] = out_weight[...]
    in_copy[...] = in_gain[...]
    mid_copy[...] = mid_gain[...]
    ready = ready_of(own[...], in_gain)
    left[...] = gated(ready, left_pair, own.shape)
    right[...] = gated(ready, right_pair, own.shape)
    gate[...] = jax.nn.sigmoid(dot32(ready, out_gate[...])).reshape(own.shape)


def near_kernel(
    left, own_right, own_other, far, in_gain, left_pair, right_pair,
    sums, far_left, far_right, right, *, tiles
):
    cols, rows, channels = left.shape
    same = same_rows(tiles)

    @pl.when(same)
    def _():
        right[...] = own_right[...]
        far_right[...] = gated(ready_of(far[...], in_gain), right_pair, left.shape)

    @pl.when(jnp.logical_not(same))
    def _():
        right[...] = gated(ready_of(own_other[...], in_gain), right_pair, left.shape)

    zero = jnp.zeros((rows, channels), jnp.float32)
    for begin in range(0, rows, cols):
        for j, part in enumerate(add_lines(left, right, (zero,) * cols, begin, cols)):
            sums[begin + j] = part
    far_left[...] = gated(ready_of(far[...], in_gain), left_pair, left.shape)


def far_kernel(
    far_other, far_left, far_right, sums, in_gain, right_pair, keep, send, right, total, *, tiles
):
    cols, rows, _ = far_left.shape
    same = same_rows(tiles)

    @pl.when(same)
    def _():
        right[...] = far_right[...]

    @pl.when(jnp.logical_not(same))
    def _():
        right[...] = gated(ready_of(far_other[...], in_gain), right_pair, far_left.shape)

    for begin in range(0, rows, cols):
        first = tuple(sums[begin + j] for j in range(cols))
        for j, part in enumerate(add_lines(far_left, right, first, begin, cols)):
            total[begin + j] = part
    tile = lax.axis_index("east") % tiles
    keep[...] = total[pl.ds(tile * cols, cols)]
    send[...] = total[pl.ds((tiles - 1 - tile) * cols, cols)].astype(jnp.bfloat16)


def last_kernel(keep, other, gate, mid_gain, out_weight, out, *, scale):
    total = keep[...] + other[...].astype(jnp.float32)
    mixed = (total * scale).astype(jnp.bfloat16)
    scaled = ready_of(mixed, mid_gain)
    result = dot32(scaled, out_weight[...]).reshape(out.shape) * gate[...]
    out[...] = result.astype(jnp.bfloat16)


def kernel_call(kernel, args, outs, scratch=(), first=False, last=False):
    whole = pl.BlockSpec(memory_space=pltpu.VMEM)
    if not last:
        outs = jax.tree.map(lambda leaf: pltpu.VMEM(leaf.shape, leaf.dtype), outs)
    if not first:
        args = [pltpu.with_memory_space_constraint(arg, pltpu.VMEM) for arg in args]
    return pl.pallas_call(
        kernel,
        out_shape=outs,
        in_specs=[whole] * len(args),
        out_specs=jax.tree.map(lambda _: whole, outs),
        scratch_shapes=list(scratch),
    )(*args)


def local_halves(
    pair_state,
    in_gain,
    left_weight,
    right_weight,
    left_gate,
    right_gate,
    mid_gain,
    out_weight,
    out_gate,
    *,
    north,
    east,
):
    tiles = east // north
    own = jnp.transpose(pair_state, (1, 0, 2))
    cols, rows, channels = own.shape
    across = [(e, (e + tiles) % east) for e in range(east)]
    beside = [(e, e // tiles * tiles + tiles - 1 - e % tiles) for e in range(east)]
    over = [(n, north - 1 - n) for n in range(north)]
    needed = [
        (n * east + e, (north - 1 - n) * east + e)
        for n in range(north)
        for e in range(n * tiles, n * tiles + tiles)
    ]
    wide = jax.ShapeDtypeStruct(own.shape, jnp.float32)
    square = jax.ShapeDtypeStruct((rows, rows, channels), jnp.float32)
    slim = jax.ShapeDtypeStruct(own.shape, jnp.bfloat16)
    line = jax.ShapeDtypeStruct((1, channels), jnp.float32)
    weight = jax.ShapeDtypeStruct(out_weight.shape, jnp.bfloat16)
    double = jax.ShapeDtypeStruct((channels, 2 * channels), jnp.bfloat16)
    far = lax.ppermute(own, "east", across)
    own_other = lax.ppermute(own, "north", over)
    far_other = lax.ppermute(far, ("north", "east"), needed)
    left, right, gate, left_pair, right_pair, out_copy, in_copy, mid_copy = kernel_call(
        own_kernel,
        (own, in_gain[None], left_weight, right_weight, left_gate, right_gate)
        + (mid_gain[None], out_weight, out_gate),
        (wide, wide, wide, double, double, weight, line, line),
        first=True,
    )
    sums, far_left, far_right = kernel_call(
        functools.partial(near_kernel, tiles=tiles),
        (left, right, own_other, far, in_copy, left_pair, right_pair),
        (square, wide, wide),
        (pltpu.VMEM(own.shape, jnp.float32),),
    )
    keep, send = kernel_call(
        functools.partial(far_kernel, tiles=tiles),
        (far_other, far_left, far_right, sums, in_copy, right_pair),
        (wide, slim),
        (pltpu.VMEM(own.shape, jnp.float32), pltpu.VMEM(square.shape, jnp.float32)),
    )
    other = lax.ppermute(send, "east", beside)
    result = kernel_call(
        functools.partial(last_kernel, scale=(cols * east) ** (-0.5)),
        (keep, other, gate, mid_copy, out_copy),
        slim,
        last=True,
    )
    return jnp.transpose(result, (1, 0, 2))


def takes_halves(north, east):
    return north == 2 and east == 2 * north


def pick_local(pair_state, *rest, north, east):
    rows, cols, _ = pair_state.shape
    small = pair_state.size * pair_state.dtype.itemsize * east <= 2**21
    if small and takes_halves(north, east) and rows == 2 * cols:
        return local_halves(pair_state, *rest, north=north, east=east)
    return local_lines(pair_state, *rest)


def solution(mesh):
    return jax.shard_map(
        functools.partial(pick_local, north=mesh.shape["north"], east=mesh.shape["east"]),
        mesh=mesh,
        in_specs=(
            P(("trial", "north"), "east", None),
            P(),
            P("trial", None),
            P("trial", None),
            P("trial", None),
            P("trial", None),
            P(),
            P("trial", None),
            P("trial", None),
        ),
        out_specs=P(("trial", "north"), "east", None),
        check_vma=False,
    )
```
